16 devices in a mesh: dp: 4 (over y, z, core), sp: 4 (over x).
Axes of the slice: x: 4, y: 2, z: 1, core: 2. Of those that a mesh axis runs over, the one named last changes fastest.
The devices are a block of a 4x4x8 slice.
Arguments:
- q: bfloat16 [128, 48, 256], P('dp'), parts along dimension 0
- k: bfloat16 [128, 8192, 1, 256], P('dp', 'sp'), parts along dimension 0
- v: bfloat16 [128, 8192, 1, 256], P('dp', 'sp'), parts along dimension 0
Outputs:
- q: bfloat16 [128, 48, 256], P('dp'), parts along dimension 0
There are 4 independent parts. The reference program is written for one: setup_inputs(seed, part) draws one part's arguments, and reference() takes and returns one part's arrays. A program takes and returns all parts, laid end to end along the dimension named above; each array names one.
All inputs are finite; a program needn't handle non-finite values.
Results may differ from the reference program's by a relative error of at most 0.012.
Values are sent between devices in bfloat16 or wider.
A program may use at most 768 MiB of HBM per device.

```python
import jax
import jax.numpy as jnp

BATCH = 32
CACHE = 8192
HEADS = 48
KV_HEADS = 1
HEAD = 256


def setup_inputs(seed: int = 0, part: int = 0) -> dict:
    kq, kk, kv = (jax.random.fold_in(k, part) for k in jax.random.split(jax.random.key(seed), 3))
    return {
        "q": (3 * jax.random.normal(kq, (BATCH, HEADS, HEAD), jnp.float32)).astype(jnp.bfloat16),
        "k": jax.random.normal(kk, (BATCH, CACHE, KV_HEADS, HEAD), jnp.float32).astype(jnp.bfloat16),
        "v": jax.random.normal(kv, (BATCH, CACHE, KV_HEADS, HEAD), jnp.float32).astype(jnp.bfloat16),
    }


def einsum(form, a, b):
    return jnp.einsum(form, a.astype(jnp.float32), b.astype(jnp.float32))


def reference(q, k, v):
    grouped = q.reshape(BATCH, KV_HEADS, -1, HEAD)
    scores = einsum("bgsd,bugd->bgsu", grouped, k) * HEAD**-0.5
    weights = jax.nn.softmax(scores, -1).astype(jnp.bfloat16)
    return einsum("bgsu,bugd->bgsd", weights, v).astype(jnp.bfloat16).reshape(BATCH, HEADS, HEAD)
```

```python
import functools
import math

import jax
import jax.numpy as jnp
from jax import lax
from jax.experimental import pallas as pl
from jax.experimental.pallas import tpu as pltpu
from jax.sharding import PartitionSpec as P

MESH = pl.DeviceIdType.MESH
F32, BF16 = jnp.float32, jnp.bfloat16
SLOTS = 8
RUN = 256


def kernel(n, scale, q_hbm, k_hbm, v_hbm, out, qbuf, kbuf, vbuf, score, top, own, part, stat, got, got_stat, qsem, ksem, vsem, psend, precv, ssend, srecv, asend, arecv):
    count, heads, head = q_hbm.shape
    keys = k_hbm.shape[1]
    groups = count // n
    runs = keys // RUN
    me, dp = lax.axis_index("sp"), lax.axis_index("dp")
    peer = [lax.rem(me + o, n) for o in range(n)]

    def k_copy(i, slot):
        return pltpu.make_async_copy(k_hbm.at[i], kbuf.at[slot], ksem.at[slot])

    def v_copy(i, slot):
        return pltpu.make_async_copy(v_hbm.at[i], vbuf.at[slot], vsem.at[slot])

    q_copy = pltpu.make_async_copy(q_hbm, qbuf, qsem)
    k_copy(0, 0).start(priority=1)
    q_copy.start(priority=1)
    v_copy(0, 0).start(priority=1)
    for i in range(1, SLOTS):
        k_copy(i, i).start(priority=1)
        v_copy(i, i).start(priority=1)
    barrier = pltpu.get_barrier_semaphore()
    for o in range(1, n):
        pl.semaphore_signal(barrier, inc=1, device_id=(dp, peer[o]), device_id_type=MESH)

    rows = lax.broadcasted_iota(jnp.int32, (heads, 128), 0)
    lanes = lax.broadcasted_iota(jnp.int32, (heads, 128), 1)
    diagonal = rows == lanes

    def as_row(column):
        return jnp.sum(jnp.where(diagonal, column, 0.0), 0, keepdims=True)

    def as_column(row):
        return jnp.sum(jnp.where(diagonal, row, 0.0), 1, keepdims=True)

    def both(a, a_slot, a_par, b, b_slot, b_par):
        if b is not None:
            high = jnp.max(top[b_par], 1, keepdims=True)
            total = jnp.zeros((heads, 128), F32)
            seen = jnp.zeros((heads, head), F32)
        largest = None
        if a is not None:
            q = qbuf[a]
        for r in range(runs):
            at = pl.ds(r * RUN, RUN)
            if a is not None:
                s = lax.dot_general(q, kbuf[a_slot, at, :], (((1,), (1,)), ((), ())), preferred_element_type=F32)
                score[a_par, :, at] = s
                m = functools.reduce(jnp.maximum, [s[:, c : c + 128] for c in range(0, RUN, 128)])
                largest = m if largest is None else jnp.maximum(largest, m)
            if b is not None:
                w = jnp.exp2((score[b_par, :, at] - high) * scale)
                for c in range(0, RUN, 128):
                    total += w[:, c : c + 128]
                seen += jnp.dot(w.astype(BF16), vbuf[b_slot, at, :], preferred_element_type=F32)
        if a is not None:
            top[a_par] = largest
        if b is not None:
            own[b] = seen
            part[b] = seen.astype(BF16)
            stat[b, 0:1] = as_row(high)
            stat[b, 1:2] = as_row(jnp.sum(total, 1, keepdims=True))

    def part_copies(g, o):
        i = g * n + peer[o]
        to = (dp, peer[o])
        return (
            pltpu.make_async_remote_copy(part.at[i], got.at[g, o - 1], psend.at[g, o - 1], precv.at[g, o - 1], device_id=to, device_id_type=MESH),
            pltpu.make_async_remote_copy(stat.at[i], got_stat.at[g, o - 1], ssend.at[g, o - 1], srecv.at[g, o - 1], device_id=to, device_id_type=MESH),
        )

    def result_copy(g, o):
        i = g * n + me
        return pltpu.make_async_remote_copy(out.at[i], out.at[i], asend.at[g, o - 1], arecv.at[g, o - 1], device_id=(dp, peer[o]), device_id_type=MESH)

    def send_parts(g):
        for o in range(1, n):
            for copy in part_copies(g, o):
                copy.start()

    def combine(i, parts, stats):
        highs, totals = [s[0:1] for s in stats], [s[1:2] for s in stats]
        most = functools.reduce(jnp.maximum, highs)
        ws = [jnp.exp2((h - most) * scale) for h in highs]
        whole = sum(t * w for t, w in zip(totals, ws))
        out[i] = sum(p.astype(F32) * as_column(w / whole) for p, w in zip(parts, ws)).astype(BF16)

    def finish(g):
        i = g * n + me
        for o in range(1, n):
            for copy in part_copies(g, o):
                copy.wait_recv()
        combine(i, [own[i]] + [got[g, o] for o in range(n - 1)], [stat[i]] + [got_stat[g, o] for o in range(n - 1)])
        for o in range(1, n):
            result_copy(g, o).start()

    def advance(i, slot, next_slot, par, last=False):
        if not last:
            k_copy(i + 1, next_slot).wait()
        v_copy(i, slot).wait()
        both(None if last else i + 1, next_slot, 1 - par, i, slot, par)

    q_copy.wait()
    k_copy(0, 0).wait()
    both(0, 0, 0, None, None, None)
    k_copy(SLOTS, 0).start(priority=1)

    def group(g, carry):
        for j in range(n):
            i = g * n + j
            slot, next_slot = lax.rem(i, SLOTS), lax.rem(i + 1, SLOTS)
            advance(i, slot, next_slot, j % 2)

            @pl.when(i + 1 + SLOTS < count)
            def _():
                k_copy(i + 1 + SLOTS, next_slot).start(priority=1)

            @pl.when(i + SLOTS < count)
            def _():
                v_copy(i + SLOTS, slot).start(priority=1)

        @pl.when(g == 0)
        def _():
            pl.semaphore_wait(barrier, n - 1)

        send_parts(g)

        @pl.when(g > 0)
        def _():
            finish(g - 1)

        return carry

    last = groups - 1
    lax.fori_loop(0, last, group, 0)

    def tail_copies(j, o):
        i = last * n + j
        to = (dp, peer[o])
        at = last + j
        return (
            pltpu.make_async_remote_copy(part.at[i], got.at[at, o - 1], psend.at[at, o - 1], precv.at[at, o - 1], device_id=to, device_id_type=MESH),
            pltpu.make_async_remote_copy(stat.at[i], got_stat.at[at, o - 1], ssend.at[at, o - 1], srecv.at[at, o - 1], device_id=to, device_id_type=MESH),
        )

    for j in range(n):
        i = last * n + j
        advance(i, i % SLOTS, (i + 1) % SLOTS, j % 2, last=j == n - 1)
        for o in range(1, n):
            for copy in tail_copies(j, o):
                copy.start()
        if j == 0:
            finish(last - 1)
    for j in range(n):
        i = last * n + j
        at = last + j
        for o in range(1, n):
            for copy in tail_copies(j, o):
                copy.wait_recv()
        combine(i, [own[i]] + [got[at, o] for o in range(n - 1)], [stat[i]] + [got_stat[at, o] for o in range(n - 1)])

    def drain(g, carry):
        for o in range(1, n):
            for copy in part_copies(g, o):
                copy.wait_send()
            result_copy(g, o).wait()
        return carry

    lax.fori_loop(0, last, drain, 0)
    for j in range(n):
        for o in range(1, n):
            for copy in tail_copies(j, o):
                copy.wait_send()


def attend(n, q, k, v):
    count, heads, head = q.shape
    keys = k.shape[1]
    q = pltpu.with_memory_space_constraint(q, pltpu.HBM)
    k, v = k.reshape(count, keys, head), v.reshape(count, keys, head)
    scale = head**-0.5 * math.log2(math.e)
    groups = count // n
    slots = groups - 1 + n
    dma = pltpu.SemaphoreType.DMA
    return pl.pallas_call(
        functools.partial(kernel, n, scale),
        out_shape=jax.ShapeDtypeStruct(q.shape, q.dtype),
        in_specs=[pl.BlockSpec(memory_space=pltpu.HBM)] * 3,
        out_specs=pl.BlockSpec(memory_space=pltpu.VMEM),
        scratch_shapes=[
            pltpu.VMEM((count, heads, head), BF16),
            pltpu.VMEM((SLOTS, keys, head), BF16),
            pltpu.VMEM((SLOTS, keys, head), BF16),
            pltpu.VMEM((2, heads, keys), F32),
            pltpu.VMEM((2, heads, 128), F32),
            pltpu.VMEM((count, heads, head), F32),
            pltpu.VMEM((count, heads, head), BF16),
            pltpu.VMEM((count, 2, 128), F32),
            pltpu.VMEM((slots, n - 1, heads, head), BF16),
            pltpu.VMEM((slots, n - 1, 2, 128), F32),
            dma,
            dma((SLOTS,)),
            dma((SLOTS,)),
            dma((slots, n - 1)),
            dma((slots, n - 1)),
            dma((slots, n - 1)),
            dma((slots, n - 1)),
            dma((groups - 1, n - 1)),
            dma((groups - 1, n - 1)),
        ],
        compiler_params=pltpu.CompilerParams(collective_id=0, has_side_effects=True, vmem_limit_bytes=52 * 2**20),
    )(q, k, v)


def solution(mesh):
    return jax.shard_map(
        functools.partial(attend, mesh.shape["sp"]),
        mesh=mesh,
        in_specs=(P("dp", None, None), P("dp", "sp", None, None), P("dp", "sp", None, None)),
        out_specs=P("dp", None, None),
        check_vma=False,
    )
```

```python
import functools
import math

import jax
import jax.numpy as jnp
from jax import lax
from jax.experimental import pallas as pl
from jax.experimental.pallas import tpu as pltpu
from jax.sharding import PartitionSpec as P

MESH = pl.DeviceIdType.MESH
F32, BF16 = jnp.float32, jnp.bfloat16
SLOTS = 8
DEPTH = 4
RUN = 256
GAP = 11
LATE = 4
HEAD, BLOCK, TAIL = 0, 2, 4


def plan(groups, n):
    away = [n // 2] + [o for o in range(1, n) if o != n // 2]
    others = [(g, o) for g in range(groups) for o in away]
    order, used = [], 0
    for g in range(groups):
        until = len(others) if g >= groups - LATE else min(g * (n - 1) + GAP, len(others))
        order += others[used:until] + [(g, 0)]
        used = until
    return order


def split(steps):
    sizes = [1] * HEAD + [BLOCK] * ((steps - HEAD - TAIL) // BLOCK)
    sizes += [1] * (steps - sum(sizes))
    ends = [sum(sizes[: i + 1]) for i in range(len(sizes))]
    return [list(range(e - z, e)) for e, z in zip(ends, sizes)]


def kernel(n, scale, q_hbm, k_hbm, v_hbm, out, qbuf, kbuf, vbuf, score, top, part, stat, got, got_stat, qsem, ksem, vsem, psend, precv, ssend, srecv, asend, arecv):
    count, heads, head = q_hbm.shape
    keys = k_hbm.shape[1]
    groups = count // n
    me, dp = lax.axis_index("sp"), lax.axis_index("dp")
    peer = [lax.rem(me + o, n) for o in range(n)]
    order = plan(groups, n)
    seq = [g * n + peer[o] for g, o in order]

    def k_copy(t):
        return pltpu.make_async_copy(k_hbm.at[seq[t]], kbuf.at[t % SLOTS], ksem.at[t % SLOTS])

    def v_copy(t):
        return pltpu.make_async_copy(v_hbm.at[seq[t]], vbuf.at[t % SLOTS], vsem.at[t % SLOTS])

    q_copy = pltpu.make_async_copy(q_hbm, qbuf, qsem)
    k_copy(0).start(priority=0)
    q_copy.start(priority=0)
    k_copy(1).start(priority=0)
    v_copy(0).start(priority=1)
    v_copy(1).start(priority=1)
    for t in range(2, SLOTS):
        k_copy(t).start(priority=1)
        v_copy(t).start(priority=1)
    barrier = pltpu.get_barrier_semaphore()
    for o in range(1, n):
        pl.semaphore_signal(barrier, inc=1, device_id=(dp, peer[o]), device_id_type=MESH)

    rows = lax.broadcasted_iota(jnp.int32, (heads, heads), 0)
    lanes = lax.broadcasted_iota(jnp.int32, (heads, heads), 1)
    diagonal = rows == lanes

    def as_column(row):
        return jnp.sum(jnp.where(diagonal, row, 0.0), 1, keepdims=True)

    def attend(ahead, now):
        largest = {}
        high = {b: jnp.max(top[b % DEPTH], 0, keepdims=True) for b in now}
        total = {b: jnp.zeros((8, heads), F32) for b in now}
        seen = {b: jnp.zeros((heads, head), F32) for b in now}
        for r in range(keys // RUN):
            at = pl.ds(r * RUN, RUN)
            for a in ahead:
                s = lax.dot_general(kbuf[a % SLOTS, at, :], qbuf[seq[a]], (((1,), (1,)), ((), ())), preferred_element_type=F32)
                score[a % DEPTH, at, :] = s
                m = jnp.max(s.reshape(RUN // 8, 8, heads), 0)
                largest[a] = m if r == 0 else jnp.maximum(largest[a], m)
            for b in now:
                w = jnp.exp2((score[b % DEPTH, at, :] - high[b]) * scale)
                total[b] += jnp.sum(w.reshape(RUN // 8, 8, heads), 0)
                seen[b] += lax.dot_general(w.astype(BF16), vbuf[b % SLOTS, at, :], (((0,), (0,)), ((), ())), preferred_element_type=F32)
        for a in ahead:
            top[a % DEPTH] = largest[a]
        return [(seen[b], high[b], jnp.sum(total[b], 0, keepdims=True)) for b in now]

    def part_copies(g, o):
        to = (dp, peer[o])
        return (
            pltpu.make_async_remote_copy(part.at[g, o - 1], got.at[g, o - 1], psend.at[g, o - 1], precv.at[g, o - 1], device_id=to, device_id_type=MESH),
            pltpu.make_async_remote_copy(stat.at[g, o - 1], got_stat.at[g, o - 1], ssend.at[g, o - 1], srecv.at[g, o - 1], device_id=to, device_id_type=MESH),
        )

    def result_copy(g, o):
        i = g * n + me
        return pltpu.make_async_remote_copy(out.at[i], out.at[i], asend.at[g, o - 1], arecv.at[g, o - 1], device_id=(dp, peer[o]), device_id_type=MESH)

    def finish(g, seen, high, total):
        i = g * n + me
        for o in range(1, n):
            for copy in part_copies(g, o):
                copy.wait_recv()
        parts = [seen] + [got[g, o] for o in range(n - 1)]
        highs = [high] + [got_stat[g, o, 0:1] for o in range(n - 1)]
        totals = [total] + [got_stat[g, o, 1:2] for o in range(n - 1)]
        most = functools.reduce(jnp.maximum, highs)
        ws = [jnp.exp2((h - most) * scale) for h in highs]
        whole = sum(t * w for t, w in zip(totals, ws))
        out[i] = sum(p.astype(F32) * as_column(w / whole) for p, w in zip(parts, ws)).astype(BF16)
        pending.extend(result_copy(g, o) for o in (2, 1, 3))
        if g >= groups - LATE - 1:
            while pending:
                pending.pop(0).start()

    steps = len(order)
    blocks = split(steps)
    pending = []
    q_copy.wait()
    for t in blocks[0]:
        k_copy(t).wait()
    attend(blocks[0], [])
    for i, now in enumerate(blocks):
        ahead = blocks[i + 1] if i + 1 < len(blocks) else []
        for t in now:
            if t + SLOTS < steps:
                k_copy(t + SLOTS).start(priority=1)
        for t in ahead:
            k_copy(t).wait()
        for t in now:
            v_copy(t).wait()
        found = attend(ahead, now)
        for t, (seen, high, total) in zip(now, found):
            g, o = order[t]
            if t + SLOTS < steps:
                v_copy(t + SLOTS).start(priority=1)
            if o:
                part[g, o - 1] = seen.astype(BF16)
                stat[g, o - 1, 0:1] = high
                stat[g, o - 1, 1:2] = total
                if t == 0:
                    pl.semaphore_wait(barrier, n - 1)
                for copy in part_copies(g, o):
                    copy.start()
                if pending:
                    pending.pop(0).start()
            else:
                finish(g, seen, high, total)

    def drain(g, carry):
        for o in range(1, n):
            for copy in part_copies(g, o):
                copy.wait_send()
            result_copy(g, o).wait()
        return carry

    lax.fori_loop(0, groups, drain, 0)


def attention(n, q, k, v):
    count, heads, head = q.shape
    keys = k.shape[1]
    q = pltpu.with_memory_space_constraint(q, pltpu.HBM)
    k, v = k.reshape(count, keys, head), v.reshape(count, keys, head)
    scale = head**-0.5 * math.log2(math.e)
    groups = count // n
    dma = pltpu.SemaphoreType.DMA
    return pl.pallas_call(
        functools.partial(kernel, n, scale),
        out_shape=jax.ShapeDtypeStruct(q.shape, q.dtype),
        in_specs=[pl.BlockSpec(memory_space=pltpu.HBM)] * 3,
        out_specs=pl.BlockSpec(memory_space=pltpu.VMEM),
        scratch_shapes=[
            pltpu.VMEM((count, heads, head), BF16),
            pltpu.VMEM((SLOTS, keys, head), BF16),
            pltpu.VMEM((SLOTS, keys, head), BF16),
            pltpu.VMEM((DEPTH, keys, heads), F32),
            pltpu.VMEM((DEPTH, 8, heads), F32),
            pltpu.VMEM((groups, n - 1, heads, head), BF16),
            pltpu.VMEM((groups, n - 1, 2, heads), F32),
            pltpu.VMEM((groups, n - 1, heads, head), BF16),
            pltpu.VMEM((groups, n - 1, 2, heads), F32),
            dma,
            dma((SLOTS,)),
            dma((SLOTS,)),
        ]
        + [dma((groups, n - 1))] * 6,
        compiler_params=pltpu.CompilerParams(collective_id=0, has_side_effects=True, vmem_limit_bytes=52 * 2**20),
    )(q, k, v)


def solution(mesh):
    return jax.shard_map(
        functools.partial(attention, mesh.shape["sp"]),
        mesh=mesh,
        in_specs=(P("dp", None, None), P("dp", "sp", None, None), P("dp", "sp", None, None)),
        out_specs=P("dp", None, None),
        check_vma=False,
    )
```
